32 devices in a mesh: row: 4 (over z), col: 8 (over y, x, core).
Axes of the slice: x: 2, y: 2, z: 4, core: 2. Of those that a mesh axis runs over, the one named last changes fastest.
Arguments:
- response_coeffs: float32 [3, 8192, 1024], P(None, ('row', 'col')), may hold values from -6 to 6
- occupied_coeffs: float32 [8192, 1024], P(('row', 'col')), may hold values from -0.1875 to 0.1875
Outputs:
- density: float32 [3, 8192, 8192], P(None, 'row', 'col')
The draws below stay inside these ranges and needn't reach their ends.
All inputs are finite; a program needn't handle non-finite values.
Results may differ from the reference program's by a relative error of at most 0.0003.
Values sent between devices are 32-bit elements; how exact they have to be, the bound alone decides.
A program may use at most 256 MiB of HBM per device.

```python
import jax
import jax.numpy as jnp
from jax import lax

BASIS = 8192
OCC = 1024
PERTURB = 3


def level_of(key, dims, split, low, top_value):
    gain, own = 1.0, jax.random.fold_in(key, 6)
    for dim, blocks in split:
        heights = jnp.exp(jax.random.uniform(jax.random.fold_in(own, dim), (blocks,), jnp.float32, low / len(split), top_value / len(split)))
        gain = gain * jnp.repeat(heights, dims[dim] // blocks).reshape([-1 if axis == dim else 1 for axis in range(len(dims))])
    return gain


def normal_values(rng, shape, deviation, most, pieces=(), dtype=jnp.bfloat16):
    values = deviation * jax.random.normal(rng, shape, jnp.float32)
    if pieces:
        values = values * level_of(rng, shape, pieces, -0.22, 0.18)
    return jnp.clip(values, -most, most).astype(dtype)


def setup_inputs(seed: int = 0) -> dict:
    keys = jax.random.split(jax.random.key(seed), 3)
    response_coeffs = normal_values(keys[0], (PERTURB, BASIS, OCC), 1.0, 6.0, ((1, 32),), jnp.float32)
    occupied_coeffs = normal_values(keys[1], (BASIS, OCC), OCC ** -0.5, 0.1875, ((0, 32),), jnp.float32)
    return dict(response_coeffs=response_coeffs, occupied_coeffs=occupied_coeffs)


SLICE_PAIRS = ((0, 0), (0, 1), (1, 0))


def split_slices(values):
    leading = lax.optimization_barrier(values.astype(jnp.bfloat16))
    remainder = values - leading.astype(jnp.float32)
    trailing = lax.optimization_barrier(remainder.astype(jnp.bfloat16))
    return [leading, trailing]


def reference(response_coeffs, occupied_coeffs):
    response_slices = split_slices(response_coeffs)
    occupied_slices = split_slices(occupied_coeffs)
    accumulated = jnp.zeros((PERTURB, BASIS, BASIS), jnp.float32)
    for left_index, right_index in SLICE_PAIRS:
        accumulated = accumulated + jnp.einsum(
            "kno,mo->knm",
            response_slices[left_index].astype(jnp.float32),
            occupied_slices[right_index].astype(jnp.float32),
            precision=lax.Precision.HIGHEST,
        )
    return accumulated + jnp.swapaxes(accumulated, 1, 2)
```

```python
import functools

import jax
import jax.numpy as jnp
from jax import lax
from jax.experimental import pallas as pl
from jax.experimental.pallas import tpu as pltpu
from jax.sharding import PartitionSpec as P

SLICE_PAIRS = ((0, 0), (0, 1), (1, 0))


def partner(value, axis, stride):
    mask = 2**stride
    pairs = [(source, source ^ mask) for source in range(lax.axis_size(axis))]
    return lax.ppermute(value, axis, pairs)


def split_slices(values):
    leading = lax.optimization_barrier(values.astype(jnp.bfloat16))
    remainder = values - leading.astype(jnp.float32)
    trailing = lax.optimization_barrier(remainder.astype(jnp.bfloat16))
    return [leading, trailing]


def contribute(row_slices, column_slices, perturbations):
    accumulated = jnp.zeros(
        (perturbations, row_slices[0].shape[1], column_slices[0].shape[1]), jnp.float32
    )
    for left_index, right_index in SLICE_PAIRS:
        forward_term = jnp.einsum(
            "kro,co->krc",
            row_slices[left_index][:perturbations],
            column_slices[right_index][perturbations],
            preferred_element_type=jnp.float32,
        )
        mirror_term = jnp.einsum(
            "ro,kco->krc",
            row_slices[right_index][perturbations],
            column_slices[left_index][:perturbations],
            preferred_element_type=jnp.float32,
        )
        accumulated = accumulated + forward_term + mirror_term
    return accumulated


def relay_columns(stacked, perturbations):
    rows_total = lax.axis_size("row")
    columns_total = lax.axis_size("col")
    col_index = lax.axis_index("col")
    shard_rows = stacked.shape[1]
    orbitals = stacked.shape[2]
    half_rows = shard_rows // 2
    swap_bit = rows_total.bit_length() - 1
    own_first = stacked[:, :half_rows]
    partner_second = partner(stacked[:, half_rows:], "col", swap_bit)
    even_first = col_index // rows_total == 0
    leading = jnp.where(even_first, own_first, partner_second)
    trailing = jnp.where(even_first, partner_second, own_first)
    paired = jnp.concatenate([leading, trailing], axis=1)
    gathered = lax.all_gather(paired, "row", axis=1, tiled=True)
    regrouped = lax.all_to_all(gathered, "col", split_axis=1, concat_axis=1, tiled=True)
    shaped = regrouped.reshape(perturbations + 1, 2, rows_total, half_rows, orbitals)
    flipped = shaped[:, ::-1]
    ordered = jnp.where(col_index % 2 == 0, shaped, flipped)
    return jnp.swapaxes(ordered, 1, 2).reshape(
        perturbations + 1, columns_total * half_rows, orbitals
    )


def shards(response_coeffs, occupied_coeffs):
    perturbations = response_coeffs.shape[0]
    stacked = jnp.concatenate([response_coeffs, occupied_coeffs[None]], axis=0)
    column_panel = relay_columns(stacked, perturbations)
    column_slices = split_slices(column_panel)
    return contribute(
        split_slices(lax.all_gather(stacked, "col", axis=1, tiled=True)),
        column_slices,
        perturbations,
    )


CUTS = 4


def flip(value):
    return value + 1 - 2 * (value % 2)


def across(value):
    return value + 2 - 4 * (value // 2)


def panel_kernel(
    resp, occ, out, rowbuf, colbuf, straybuf,
    row_lead, row_trail, col_lead, col_trail, stage, acc,
    rx_row, rx_col, rx_stray, tx, stage_sem, acc_sem,
):
    perturbations, shard_rows, orbitals = resp.shape
    kinds = perturbations + 1
    cut = shard_rows // CUTS
    pieces = kinds * CUTS
    early = pieces // 2
    panel_rows = 8 * shard_rows
    block_rows = 2 * shard_rows
    row_blocks = panel_rows // block_rows

    z = lax.axis_index("row")
    planes = lax.axis_size("row")
    column = lax.axis_index("col")
    w, core = column // 2, column % 2
    xq, yq, dq = flip(w), across(w), flip(across(w))
    other = 1 - core
    x_dev, y_dev, p_dev = (z, 2 * xq + core), (z, 2 * yq + core), (z, 2 * w + other)
    up_dev, down_dev = (z + 1, column), (z - 1, column)
    has_up, has_down = z < planes - 1, z > 0
    diagonal = z == w
    match = w // 2 == core
    distance = jnp.where(z > w, z - w, w - z)

    lone = ((z > w) & (core == 1)) | ((z < w) & (core == 0))
    total_up = jnp.where(core == 0, 4 * pieces, 2 * pieces)
    total_down = jnp.where(core == 1, 4 * pieces, 2 * pieces)
    total_in = jnp.where(lone, 2 * pieces, 4 * pieces)

    rising = w == 3
    outer = rising | (w == 0)
    depth = jnp.where(rising, z, planes - 1 - z)
    side = jnp.where(rising, core, other)
    lone_core = jnp.where(rising, 1, 0)
    onward_dev = (jnp.where(rising, z + 1, z - 1), column)
    inbound = outer & (depth > 0)
    onward = outer & (depth < planes - 1)
    relay = ((w == 1) & (core == 1)) | ((w == 2) & (core == 0))

    barrier = pltpu.get_barrier_semaphore()

    def greet(device):
        pl.semaphore_signal(barrier, inc=1, device_id=device, device_id_type=pl.DeviceIdType.MESH)

    for device in (x_dev, y_dev, p_dev, (z, 2 * xq + other), (z, 2 * yq + other)):
        greet(device)

    @pl.when(has_up)
    def _():
        greet(up_dev)

    @pl.when(has_down)
    def _():
        greet(down_dev)

    pl.semaphore_wait(barrier, 5 + jnp.where(has_up, 1, 0) + jnp.where(has_down, 1, 0))

    def rows_at(j):
        return pl.ds(pl.multiple_of((j % CUTS) * cut, cut), cut)

    def row_piece(quarter, lane, j):
        return rowbuf.at[2 * quarter + lane, j // CUTS, rows_at(j)]

    def col_piece(p):
        i, j = p // pieces, p % pieces
        return colbuf.at[i, j // CUTS, rows_at(j)]

    def stray_piece(q, j):
        return straybuf.at[q, j // CUTS, rows_at(j)]

    def send(source, target, send_sem, recv_sem, device):
        pltpu.make_async_remote_copy(
            src_ref=source, dst_ref=target, send_sem=send_sem, recv_sem=recv_sem,
            device_id=device, device_id_type=pl.DeviceIdType.MESH,
        ).start()

    def send_row(quarter, lane, j, slot, device):
        ref = row_piece(quarter, lane, j)
        send(ref, ref, tx.at[slot], rx_row.at[2 * quarter + lane, j], device)

    def arrived(ref, sem):
        pltpu.make_async_copy(ref, ref, sem).wait()

    def wait_row(quarter, lane, j):
        arrived(row_piece(quarter, lane, j), rx_row.at[2 * quarter + lane, j])

    def wait_col(p):
        arrived(col_piece(p), rx_col.at[p])

    load_resp = pltpu.make_async_copy(resp, stage.at[pl.ds(1, perturbations)], stage_sem.at[0])
    load_occ = pltpu.make_async_copy(occ, stage.at[0], stage_sem.at[1])
    load_resp.start()
    load_occ.start()

    def launch(source, j):
        for slot, device in ((0, x_dev), (1, y_dev), (4, p_dev)):
            send(source, row_piece(w, core, j), tx.at[slot], rx_row.at[2 * w + core, j], device)

        @pl.when(diagonal & match & has_up)
        def _():
            send(source, col_piece(j), tx.at[5], rx_col.at[j], up_dev)

        @pl.when(diagonal & match & has_down)
        def _():
            send(source, col_piece(j), tx.at[6], rx_col.at[j], down_dev)

        @pl.when(outer & ((depth == 0) | ((depth == 2) & (side == 1))))
        def _():
            send(source, stray_piece(depth, j), tx.at[7], rx_stray.at[depth, j], onward_dev)

    def launch_occ(j, carry):
        launch(occ.at[rows_at(j)], j)
        return carry

    def launch_resp(j, carry):
        launch(resp.at[j // CUTS - 1, rows_at(j)], j)
        return carry

    lax.fori_loop(0, CUTS, launch_occ, 0)
    lax.fori_loop(CUTS, pieces, launch_resp, 0)
    load_resp.wait()
    load_occ.wait()
    keep = pltpu.make_async_copy(stage, rowbuf.at[2 * w + core], stage_sem.at[0])
    keep.start()
    keep.wait()

    first = jnp.where(match, w, yq)
    second = flip(first)
    early_lane = jnp.where(lone, 1 - w % 2, core)

    def order(i):
        quarter = jnp.where(i < 2, first, second)
        lead = jnp.where(i < 2, core, early_lane)
        lane = jnp.where(i % 2 == 0, lead, 1 - lead)
        return quarter, lane

    def emit(source, p):
        @pl.when(has_up & (z >= w) & (p < total_up))
        def _():
            send(source, col_piece(p), tx.at[5], rx_col.at[p], up_dev)

        @pl.when(has_down & (z <= w) & (p < total_down))
        def _():
            send(source, col_piece(p), tx.at[6], rx_col.at[p], down_dev)

    def emit_own(p, carry):
        quarter, lane = order(p // pieces)
        emit(row_piece(quarter, lane, p % pieces), p)
        return carry

    def pass_on(p, carry):
        wait_col(p)
        emit(col_piece(p), p)
        return carry

    def clip(value, most):
        return jnp.minimum(jnp.maximum(value, 0), most)

    def surplus(value):
        return jnp.maximum(value, 0)

    def sent(t):
        fast = pieces + 1 + t + surplus(t - pieces + 1)
        slow = t + 1 + surplus(t - 2 * pieces + 1)
        return clip(jnp.where(match, fast, slow), 4 * pieces)

    def received(t):
        lagged = t - distance + 1
        return clip(lagged + 1 + surplus(lagged - 2 * pieces + 1), total_in)

    def stray_order(i):
        b = i // pieces
        return jnp.where((depth == 3) & (side == 1), (b + 2) % 3, b)

    last = 3 * pieces
    late = (depth == 3) & (side == 0)
    stray_shift = jnp.where(depth == 1, 1, jnp.where(late, -1, 0))

    def stray_received(t):
        extra = jnp.where(late, surplus(t - last + 1), 0)
        return clip(t + stray_shift + extra, depth * pieces)

    def stray_spread(t):
        return clip(2 * (t - pieces + 1), stray_received(t))

    def take_stray(i, carry):
        q, j = stray_order(i), i % pieces
        ref = stray_piece(q, j)
        arrived(ref, rx_stray.at[q, j])

        @pl.when(onward)
        def _():
            send(ref, ref, tx.at[7], rx_stray.at[q, j], onward_dev)

        return carry

    def late_slot(chip, lane):
        return 2 + jnp.where(lane == 1 - chip % 2, 0, 1)

    def spread_stray(i, carry):
        q, j = stray_order(i), i % pieces
        source = stray_piece(q, j)
        through = jnp.where(rising, 0, 1)

        @pl.when(q == 0)
        def _():
            chip = jnp.where(side == 0, xq, yq)
            send(source, stray_piece(through, j), tx.at[8], rx_stray.at[through, j], (z, 2 * chip + core))

        @pl.when(q > 0)
        def _():
            chip = jnp.where(q == 1, yq, xq)
            p = late_slot(chip, core) * pieces + j
            send(source, col_piece(p), tx.at[8], rx_col.at[p], (z, 2 * chip + lone_core))

        return carry

    def split_into(value, lead, trail, start):
        leading = value.astype(jnp.bfloat16)
        lead[pl.ds(start, shard_rows), :] = leading
        trail[pl.ds(start, shard_rows), :] = (value - leading.astype(jnp.float32)).astype(jnp.bfloat16)

    def acc_copy(k, start):
        return pltpu.make_async_copy(
            acc.at[k],
            out.at[k, :, pl.ds(pl.multiple_of(start, shard_rows), shard_rows)],
            acc_sem.at[k],
        )

    quanta = row_blocks + perturbations
    base = pieces + early + 3
    times = []
    for gap in (0, 1, 1, 2, 3, 3, 4, 5, 6, 6, 7, 8, 8, 9):
        times.append(base + gap)
    for gap in (11, 11, 10, 10, 9, 8, 7):
        times.append(last - gap)
    for gap in (6, 6, 5, 5, 4, 3, 1):
        times.append(last - gap)
    compute_lag = jnp.where(diagonal, 0, jnp.where(lone, 1, distance - 1))

    def done(t):
        count = 0
        for time in times:
            count = count + jnp.where(t - compute_lag >= time, 1, 0)
        return count

    def block_of(ref, kind, block):
        return ref[pl.ds(pl.multiple_of(kind * panel_rows + block * block_rows, block_rows), block_rows), :]

    def product(left, right):
        return lax.dot_general(left, right, (((1,), (1,)), ((), ())), preferred_element_type=jnp.float32)

    def total(kind, block):
        lead, trail = block_of(row_lead, kind, block), block_of(row_trail, kind, block)
        value = product(lead, col_lead[...])
        value += product(lead, col_trail[...])
        value += product(trail, col_lead[...])
        return value

    def target(block):
        return pl.ds(pl.multiple_of(block * block_rows, block_rows), block_rows)

    def quantum(g, carry):
        slot, q = g // quanta, g % quanta
        opening = q < row_blocks
        kind = jnp.where(opening, 0, q - row_blocks + 1)
        quarter, lane = order(slot)
        place = (2 * (quarter % 2) + lane) * shard_rows

        @pl.when((q == 0) | (q >= row_blocks))
        def _():
            @pl.when(lone & (slot >= 2))
            def _():
                def late_wait(j, carry):
                    wait_col(slot * pieces + kind * CUTS + j)
                    return carry

                lax.fori_loop(0, CUTS, late_wait, 0)

            def fetch(source):
                copy = pltpu.make_async_copy(source, stage.at[0], stage_sem.at[0])
                copy.start()
                copy.wait()

            @pl.when(diagonal)
            def _():
                fetch(rowbuf.at[2 * quarter + lane, kind])

            @pl.when(z != w)
            def _():
                fetch(colbuf.at[slot, kind])

            split_into(stage[0], col_lead, col_trail, 0)

        @pl.when((q == 0) & (slot >= 1))
        def _():
            for k in range(perturbations):
                acc_copy(k, place).wait()

        @pl.when(opening)
        def _():
            def start(k, carry):
                acc[k, target(q), :] = total(k + 1, q)
                return carry

            lax.fori_loop(0, perturbations, start, 0)

        @pl.when(q >= row_blocks)
        def _():
            k = q - row_blocks

            def finish(block, carry):
                acc[k, target(block), :] += total(0, block)
                return carry

            lax.fori_loop(0, row_blocks, finish, 0)
            acc_copy(k, place).start()

        return carry

    def step(t, carry):
        @pl.when(t < pieces)
        def _():
            wait_row(xq, core, t)
            send_row(xq, core, t, 4, p_dev)
            wait_row(yq, core, t)
            send_row(yq, core, t, 4, p_dev)
            wait_row(w, other, t)

            @pl.when(t < early)
            def _():
                send_row(yq, core, t, 2, x_dev)

            @pl.when(t >= early)
            def _():
                send_row(xq, core, t, 3, y_dev)

        @pl.when((t >= 1) & (t < pieces + 1))
        def _():
            wait_row(xq, other, t - 1)
            wait_row(yq, other, t - 1)

        @pl.when((t >= pieces) & (t < pieces + early))
        def _():
            for shift in (0, early):
                wait_row(dq, core, t - pieces + shift)
                send_row(dq, core, t - pieces + shift, 4, p_dev)

        @pl.when((t >= pieces + 1) & (t < pieces + early + 1))
        def _():
            for shift in (0, early):
                wait_row(dq, other, t - pieces - 1 + shift)

        @pl.when(diagonal)
        def _():
            opened = jnp.where(match, pieces, 0)
            lax.fori_loop(jnp.where(t == 0, opened, sent(t - 1)), sent(t), emit_own, 0)

        @pl.when(z != w)
        def _():
            lax.fori_loop(received(t - 1), received(t), pass_on, 0)

        @pl.when(inbound)
        def _():
            lax.fori_loop(stray_received(t - 1), stray_received(t), take_stray, 0)
            lax.fori_loop(stray_spread(t - 1), stray_spread(t), spread_stray, 0)

        @pl.when(outer & (depth == 1) & (t >= pieces) & (t < 2 * pieces))
        def _():
            j = t - pieces
            send(row_piece(xq, core, j), stray_piece(1, j), tx.at[7], rx_stray.at[1, j], onward_dev)

        @pl.when(outer & (depth == 2) & (side == 0) & (t >= 2 * pieces) & (t < 2 * pieces + early))
        def _():
            for shift in range(2):
                j = 2 * (t - 2 * pieces) + shift
                send(row_piece(w, core, j), stray_piece(2, j), tx.at[7], rx_stray.at[2, j], onward_dev)

        hop = t - pieces - early - 2

        @pl.when(relay & (hop >= 0) & (hop < pieces))
        def _():
            for through, chip, lone_at, here, slot in ((0, 0, 1, has_down, 9), (1, 3, 0, has_up, 10)):
                @pl.when(here)
                def _():
                    ref = stray_piece(through, hop)
                    arrived(ref, rx_stray.at[through, hop])
                    p = late_slot(chip, core) * pieces + hop
                    send(ref, col_piece(p), tx.at[slot], rx_col.at[p], (z, 2 * chip + lone_at))

        m = jnp.where(t < pieces + early + 1, t - pieces - 1, t - pieces - early + 5)

        @pl.when((m >= 0) & (m < 8) & ((m >= 6) == (t >= pieces + early + 1)))
        def _():
            quarter = jnp.where(m < 2, w, jnp.where(m < 4, xq, jnp.where(m < 6, yq, dq)))
            shard = 2 * quarter + m % 2
            copy = pltpu.make_async_copy(rowbuf.at[shard], stage, stage_sem.at[0])
            copy.start()
            copy.wait()

            def convert(k, carry):
                start = pl.multiple_of(k * panel_rows + shard * shard_rows, shard_rows)
                split_into(stage[k], row_lead, row_trail, start)
                return carry

            lax.fori_loop(0, kinds, convert, 0)

        lax.fori_loop(done(t - 1), done(t), quantum, 0)
        return carry

    lax.fori_loop(0, last + 2, step, 0)

    for k in range(perturbations):
        acc_copy(k, 0).wait()

    def drain(slot, ref):
        pltpu.make_async_copy(ref, ref, tx.at[slot]).wait()

    def drain_shards(slot, count, condition):
        @pl.when(condition)
        def _():
            drain(slot, rowbuf.at[pl.ds(0, count)])

    drain(0, rowbuf.at[0])
    drain(1, rowbuf.at[0])
    drain(2, rowbuf.at[0, pl.ds(0, kinds // 2)])
    drain(3, rowbuf.at[0, pl.ds(0, kinds // 2)])
    drain(4, rowbuf.at[pl.ds(0, 4)])
    drain_shards(5, 4, has_up & (z >= w) & (core == 0))
    drain_shards(5, 2, has_up & (z >= w) & (core == 1))
    drain_shards(6, 4, has_down & (z <= w) & (core == 1))
    drain_shards(6, 2, has_down & (z <= w) & (core == 0))
    for count in (1, 2, 3):
        drain_shards(7, count, outer & (depth == count - 1))
        drain_shards(8, count, outer & (depth == count))
    drain_shards(9, 1, relay & has_down)
    drain_shards(10, 1, relay & has_up)


def panels(response_coeffs, occupied_coeffs):
    perturbations, shard_rows, orbitals = response_coeffs.shape
    kinds = perturbations + 1
    pieces = kinds * CUTS
    any_space = pl.BlockSpec(memory_space=pl.ANY)
    float32, bfloat16 = jnp.float32, jnp.bfloat16
    return pl.pallas_call(
        panel_kernel,
        out_shape=(
            jax.ShapeDtypeStruct((perturbations, 8 * shard_rows, 4 * shard_rows), float32),
            jax.ShapeDtypeStruct((8, kinds, shard_rows, orbitals), float32),
            jax.ShapeDtypeStruct((4, kinds, shard_rows, orbitals), float32),
            jax.ShapeDtypeStruct((3, kinds, shard_rows, orbitals), float32),
        ),
        in_specs=[any_space] * 2,
        out_specs=(any_space,) * 4,
        scratch_shapes=[
            pltpu.VMEM((kinds * 8 * shard_rows, orbitals), bfloat16),
            pltpu.VMEM((kinds * 8 * shard_rows, orbitals), bfloat16),
            pltpu.VMEM((shard_rows, orbitals), bfloat16),
            pltpu.VMEM((shard_rows, orbitals), bfloat16),
            pltpu.VMEM((kinds, shard_rows, orbitals), float32),
            pltpu.VMEM((perturbations, 8 * shard_rows, shard_rows), float32),
            pltpu.SemaphoreType.DMA((8, pieces)),
            pltpu.SemaphoreType.DMA((4 * pieces,)),
            pltpu.SemaphoreType.DMA((3, pieces)),
            pltpu.SemaphoreType.DMA((11,)),
            pltpu.SemaphoreType.DMA((2,)),
            pltpu.SemaphoreType.DMA((perturbations,)),
        ],
        compiler_params=pltpu.CompilerParams(
            collective_id=0, has_side_effects=True, vmem_limit_bytes=66_000_000
        ),
    )(response_coeffs, occupied_coeffs)[0]


def solution(mesh):
    fits = mesh.shape["row"] == 4 and mesh.shape["col"] == 8
    return jax.shard_map(
        panels if fits else shards,
        mesh=mesh,
        in_specs=(P(None, ("row", "col"), None), P(("row", "col"), None)),
        out_specs=P(None, "row", "col"),
        check_vma=False,
    )
```

```python
import functools

import jax
import jax.numpy as jnp
from jax import lax
from jax.experimental import pallas as pl
from jax.experimental.pallas import tpu as pltpu
from jax.sharding import PartitionSpec as P

SLICE_PAIRS = ((0, 0), (0, 1), (1, 0))


def partner(value, axis, stride):
    mask = 2**stride
    pairs = [(source, source ^ mask) for source in range(lax.axis_size(axis))]
    return lax.ppermute(value, axis, pairs)


def split_slices(values):
    leading = lax.optimization_barrier(values.astype(jnp.bfloat16))
    remainder = values - leading.astype(jnp.float32)
    trailing = lax.optimization_barrier(remainder.astype(jnp.bfloat16))
    return [leading, trailing]


def contribute(row_slices, column_slices, perturbations):
    accumulated = jnp.zeros(
        (perturbations, row_slices[0].shape[1], column_slices[0].shape[1]), jnp.float32
    )
    for left_index, right_index in SLICE_PAIRS:
        forward_term = jnp.einsum(
            "kro,co->krc",
            row_slices[left_index][:perturbations],
            column_slices[right_index][perturbations],
            preferred_element_type=jnp.float32,
        )
        mirror_term = jnp.einsum(
            "ro,kco->krc",
            row_slices[right_index][perturbations],
            column_slices[left_index][:perturbations],
            preferred_element_type=jnp.float32,
        )
        accumulated = accumulated + forward_term + mirror_term
    return accumulated


def relay_columns(stacked, perturbations):
    rows_total = lax.axis_size("row")
    columns_total = lax.axis_size("col")
    col_index = lax.axis_index("col")
    shard_rows = stacked.shape[1]
    orbitals = stacked.shape[2]
    half_rows = shard_rows // 2
    swap_bit = rows_total.bit_length() - 1
    own_first = stacked[:, :half_rows]
    partner_second = partner(stacked[:, half_rows:], "col", swap_bit)
    even_first = col_index // rows_total == 0
    leading = jnp.where(even_first, own_first, partner_second)
    trailing = jnp.where(even_first, partner_second, own_first)
    paired = jnp.concatenate([leading, trailing], axis=1)
    gathered = lax.all_gather(paired, "row", axis=1, tiled=True)
    regrouped = lax.all_to_all(gathered, "col", split_axis=1, concat_axis=1, tiled=True)
    shaped = regrouped.reshape(perturbations + 1, 2, rows_total, half_rows, orbitals)
    flipped = shaped[:, ::-1]
    ordered = jnp.where(col_index % 2 == 0, shaped, flipped)
    return jnp.swapaxes(ordered, 1, 2).reshape(
        perturbations + 1, columns_total * half_rows, orbitals
    )


def shards(response_coeffs, occupied_coeffs):
    perturbations = response_coeffs.shape[0]
    stacked = jnp.concatenate([response_coeffs, occupied_coeffs[None]], axis=0)
    column_panel = relay_columns(stacked, perturbations)
    column_slices = split_slices(column_panel)
    return contribute(
        split_slices(lax.all_gather(stacked, "col", axis=1, tiled=True)),
        column_slices,
        perturbations,
    )


CUTS = 4


def flip(value):
    return value + 1 - 2 * (value % 2)


def across(value):
    return value + 2 - 4 * (value // 2)


def panel_kernel(
    resp, occ, out, rowbuf, colbuf, straybuf,
    row_lead, row_trail, col_lead, col_trail, stage, acc,
    rx_row, rx_col, rx_stray, tx, stage_sem, acc_sem,
):
    perturbations, shard_rows, orbitals = resp.shape
    kinds = perturbations + 1
    cut = shard_rows // CUTS
    pieces = kinds * CUTS
    early = pieces // 2
    panel_rows = 8 * shard_rows
    block_rows = panel_rows // 2
    row_blocks = panel_rows // block_rows

    z = lax.axis_index("row")
    planes = lax.axis_size("row")
    column = lax.axis_index("col")
    w, core = column // 2, column % 2
    xq, yq, dq = flip(w), across(w), flip(across(w))
    other = 1 - core
    x_dev, y_dev, p_dev = (z, 2 * xq + core), (z, 2 * yq + core), (z, 2 * w + other)
    up_dev, down_dev = (z + 1, column), (z - 1, column)
    has_up, has_down = z < planes - 1, z > 0
    diagonal = z == w
    match = w // 2 == core
    distance = jnp.where(z > w, z - w, w - z)

    lone = ((z > w) & (core == 1)) | ((z < w) & (core == 0))

    rising = w == 3
    outer = rising | (w == 0)
    depth = jnp.where(rising, z, planes - 1 - z)
    side = jnp.where(rising, core, other)
    lone_core = jnp.where(rising, 1, 0)
    onward_dev = (jnp.where(rising, z + 1, z - 1), column)
    inbound = outer & (depth > 0)
    onward = outer & (depth < planes - 1)
    relay = (w == 1) | (w == 2)

    barrier = pltpu.get_barrier_semaphore()

    def greet(device):
        pl.semaphore_signal(barrier, inc=1, device_id=device, device_id_type=pl.DeviceIdType.MESH)

    for device in (x_dev, y_dev, p_dev, (z, 2 * xq + other), (z, 2 * yq + other)):
        greet(device)

    @pl.when(has_up)
    def _():
        greet(up_dev)

    @pl.when(has_down)
    def _():
        greet(down_dev)

    pl.semaphore_wait(barrier, 5 + jnp.where(has_up, 1, 0) + jnp.where(has_down, 1, 0))

    def rows_at(j):
        return pl.ds(pl.multiple_of((j % CUTS) * cut, cut), cut)

    def row_piece(quarter, lane, j):
        return rowbuf.at[2 * quarter + lane, j // CUTS, rows_at(j)]

    def col_piece(slot, j):
        return colbuf.at[slot, j // CUTS, rows_at(j)]

    def stray_piece(q, j):
        return straybuf.at[q, j // CUTS, rows_at(j)]

    def send(source, target, send_sem, recv_sem, device):
        pltpu.make_async_remote_copy(
            src_ref=source, dst_ref=target, send_sem=send_sem, recv_sem=recv_sem,
            device_id=device, device_id_type=pl.DeviceIdType.MESH,
        ).start()

    def send_row(quarter, lane, j, slot, device):
        ref = row_piece(quarter, lane, j)
        send(ref, ref, tx.at[slot], rx_row.at[2 * quarter + lane, j], device)

    def arrived(ref, sem):
        pltpu.make_async_copy(ref, ref, sem).wait()

    def wait_row(quarter, lane, j):
        arrived(row_piece(quarter, lane, j), rx_row.at[2 * quarter + lane, j])

    def wait_col(slot, j):
        arrived(col_piece(slot, j), rx_col.at[slot, j])

    def send_col(source, slot, j, way, device):
        send(source, col_piece(slot, j), tx.at[way], rx_col.at[slot, j], device)

    load_resp = pltpu.make_async_copy(resp, stage.at[pl.ds(1, perturbations)], stage_sem.at[0])
    load_occ = pltpu.make_async_copy(occ, stage.at[0], stage_sem.at[1])
    load_resp.start()
    load_occ.start()

    def launch(source, j):
        for slot, device in ((0, x_dev), (1, y_dev), (4, p_dev)):
            send(source, row_piece(w, core, j), tx.at[slot], rx_row.at[2 * w + core, j], device)

        @pl.when(diagonal & match & has_up)
        def _():
            send_col(source, 0, j, 5, up_dev)

        @pl.when(diagonal & match & has_down)
        def _():
            send_col(source, 0, j, 6, down_dev)

        @pl.when(outer & ((depth == 0) | ((depth == 2) & (side == 1))))
        def _():
            send(source, stray_piece(depth, j), tx.at[7], rx_stray.at[depth, j], onward_dev)

    def launch_occ(j, carry):
        launch(occ.at[rows_at(j)], j)
        return carry

    def launch_resp(j, carry):
        launch(resp.at[j // CUTS - 1, rows_at(j)], j)
        return carry

    lax.fori_loop(0, CUTS, launch_occ, 0)
    lax.fori_loop(CUTS, pieces, launch_resp, 0)
    load_resp.wait()
    load_occ.wait()
    keep = pltpu.make_async_copy(stage, rowbuf.at[2 * w + core], stage_sem.at[0])
    keep.start()
    keep.wait()

    first = jnp.where(match, w, yq)
    second = flip(first)
    early_lane = jnp.where(lone, 1 - w % 2, core)

    def order(i):
        double_first = (i == 0) | (i == 3)
        quarter = jnp.where(lone, jnp.where(i < 2, first, second), jnp.where(double_first, first, second))
        lone_lane = jnp.where(i < 2, core, early_lane)
        lone_lane = jnp.where(i % 2 == 0, lone_lane, 1 - lone_lane)
        lane = jnp.where(lone, lone_lane, jnp.where(i < 2, core, other))
        return quarter, lane

    def chain_order(b, double):
        quarter = jnp.where(b == 0, first, jnp.where(double, second, jnp.where(b == 1, first, across(first))))
        lane = jnp.where(jnp.where(double, b == 2, b == 1), other, core)
        return quarter, lane

    def chain_slot(b, double):
        return jnp.where(double | (b < 2), b, 4)

    def emit_own(p, carry):
        b, j = p // pieces, p % pieces

        @pl.when(has_up)
        def _():
            quarter, lane = chain_order(b, core == 0)
            send_col(row_piece(quarter, lane, j), chain_slot(b, core == 0), j, 5, up_dev)

        @pl.when(has_down)
        def _():
            quarter, lane = chain_order(b, core == 1)
            send_col(row_piece(quarter, lane, j), chain_slot(b, core == 1), j, 6, down_dev)

        return carry

    def pass_on(p, carry):
        b, j = p // pieces, p % pieces
        slot = chain_slot(b, jnp.logical_not(lone))
        wait_col(slot, j)
        source = col_piece(slot, j)

        @pl.when(has_up & (z > w))
        def _():
            send_col(source, slot, j, 5, up_dev)

        @pl.when(has_down & (z < w))
        def _():
            send_col(source, slot, j, 6, down_dev)

        @pl.when(slot == 4)
        def _():
            send_col(source, 3, j, 9, p_dev)

        return carry

    def clip(value, most):
        return jnp.minimum(jnp.maximum(value, 0), most)

    last = 3 * pieces

    def sent(t):
        slow = t + 1 + jnp.maximum(t - pieces - early, 0)
        return clip(jnp.where(match, pieces + t + 1, slow), last)

    def received(t):
        return clip(t - distance + 2, last)

    def stray_order(i):
        b = i // pieces
        return jnp.where((depth == 3) & (side == 1), (b + 2) % 3, b)

    def stray_received(t):
        farthest = jnp.where(side == 1, t, jnp.where(t < 2 * pieces + 2, t - 4, t - 1))
        return clip(jnp.where(depth == 1, t + 1, jnp.where(depth == 2, t - 1, farthest)), depth * pieces)

    def take_stray(i, carry):
        q, j = stray_order(i), i % pieces
        ref = stray_piece(q, j)
        arrived(ref, rx_stray.at[q, j])

        @pl.when(onward)
        def _():
            send(ref, ref, tx.at[7], rx_stray.at[q, j], onward_dev)

        return carry

    def late_slot(chip, lane):
        return 2 + jnp.where(lane == 1 - chip % 2, 0, 1)

    through = jnp.where(rising, 0, 1)

    def spread_far(j):
        chip = jnp.where(j < early, xq, yq)
        send(stray_piece(0, j), stray_piece(through, j), tx.at[8], rx_stray.at[through, j], (z, 2 * chip + core))

    def spread_near(q, chip, j):
        send_col(stray_piece(q, j), late_slot(chip, core), j, 8, (z, 2 * chip + lone_core))

    def split_into(value, lead, trail, start):
        leading = value.astype(jnp.bfloat16)
        lead[pl.ds(start, shard_rows), :] = leading
        trail[pl.ds(start, shard_rows), :] = (value - leading.astype(jnp.float32)).astype(jnp.bfloat16)

    def acc_copy(bank, k, start):
        return pltpu.make_async_copy(
            acc.at[bank, k],
            out.at[k, :, pl.ds(pl.multiple_of(start, shard_rows), shard_rows)],
            acc_sem.at[bank, k],
        )

    quanta = 2 * perturbations
    base = pieces + early + 3
    times = [base + gap for gap in (0, 0, 1, 2, 2, 3, 4, 5, 5, 6, 7, 7)]
    times += [last - gap for gap in (12, 11, 11, 10, 10, 9, 8, 7, 4, 3, 1, 0)]
    compute_lag = jnp.where(diagonal, 0, jnp.where(lone, 1, distance - 1))

    def done(t):
        count = 0
        for time in times:
            count = count + jnp.where(t - compute_lag >= time, 1, 0)
        return count

    def block_of(ref, kind, block):
        return ref[pl.ds(pl.multiple_of(kind * panel_rows + block * block_rows, block_rows), block_rows), :]

    def product(left, right):
        return lax.dot_general(left, right, (((1,), (1,)), ((), ())), preferred_element_type=jnp.float32)

    def total(kind, block):
        lead, trail = block_of(row_lead, kind, block), block_of(row_trail, kind, block)
        value = product(lead, col_lead[...])
        value += product(lead, col_trail[...])
        value += product(trail, col_lead[...])
        return value

    def target(block):
        return pl.ds(pl.multiple_of(block * block_rows, block_rows), block_rows)

    def quantum(g, carry):
        h = g - 2 * quanta
        tail_slot = jnp.where(h < quanta, h // perturbations, h % 2) + 2
        tail_q = jnp.where(h < quanta, h % perturbations, perturbations + (h - quanta) // 2)
        slot = jnp.where(h < 0, g // quanta, tail_slot)
        q = jnp.where(h < 0, g % quanta, tail_q)
        opening = q < perturbations
        k = q % perturbations
        kind = jnp.where(opening, 0, k + 1)
        bank = slot % 2
        quarter, lane = order(slot)
        place = (2 * (quarter % 2) + lane) * shard_rows

        @pl.when((q == 0) | (q >= perturbations))
        def _():
            @pl.when((z != w) & ((slot == 3) | (lone & (slot == 2))))
            def _():
                def late_wait(j, carry):
                    wait_col(slot, kind * CUTS + j)
                    return carry

                lax.fori_loop(0, CUTS, late_wait, 0)

            def fetch(source):
                copy = pltpu.make_async_copy(source, stage.at[0], stage_sem.at[0])
                copy.start()
                copy.wait()

            @pl.when(diagonal)
            def _():
                fetch(rowbuf.at[2 * quarter + lane, kind])

            @pl.when(z != w)
            def _():
                fetch(colbuf.at[slot, kind])

            split_into(stage[0], col_lead, col_trail, 0)

        @pl.when((q == 0) & (slot >= 2))
        def _():
            for late in range(perturbations):
                acc_copy(bank, late, place).wait()

        @pl.when(opening)
        def _():
            def start(block, carry):
                acc[bank, k, target(block), :] = total(k + 1, block)
                return carry

            lax.fori_loop(0, row_blocks, start, 0)

        @pl.when(q >= perturbations)
        def _():
            def finish(block, carry):
                acc[bank, k, target(block), :] += total(0, block)
                return carry

            lax.fori_loop(0, row_blocks, finish, 0)
            acc_copy(bank, k, place).start()

        return carry

    def step(t, carry):
        @pl.when(t < pieces)
        def _():
            wait_row(xq, core, t)
            send_row(xq, core, t, 4, p_dev)
            wait_row(yq, core, t)
            send_row(yq, core, t, 4, p_dev)
            wait_row(w, other, t)

            @pl.when(t < early)
            def _():
                send_row(yq, core, t, 2, x_dev)

            @pl.when(t >= early)
            def _():
                send_row(xq, core, t, 3, y_dev)

        @pl.when((t >= 1) & (t < pieces + 1))
        def _():
            wait_row(xq, other, t - 1)
            wait_row(yq, other, t - 1)

        @pl.when((t >= pieces) & (t < pieces + early))
        def _():
            for shift in (0, early):
                wait_row(dq, core, t - pieces + shift)
                send_row(dq, core, t - pieces + shift, 4, p_dev)

        @pl.when((t >= pieces + 1) & (t < pieces + early + 1))
        def _():
            for shift in (0, early):
                wait_row(dq, other, t - pieces - 1 + shift)

        @pl.when(diagonal)
        def _():
            lax.fori_loop(sent(t - 1), sent(t), emit_own, 0)

        @pl.when(z != w)
        def _():
            lax.fori_loop(received(t - 1), received(t), pass_on, 0)

        @pl.when(inbound)
        def _():
            lax.fori_loop(stray_received(t - 1), stray_received(t), take_stray, 0)
            far = t - pieces - 2
            near = t - pieces - early - 2
            near_x = near - jnp.where(side == 0, early, 0)
            near_y = near - jnp.where(side == 1, early, 0)

            @pl.when((far >= 0) & (far < pieces))
            def _():
                spread_far(far)

            @pl.when((depth > 1) & (near_y >= 0) & (near_y < pieces))
            def _():
                spread_near(1, yq, near_y)

            @pl.when((depth > 2) & (near_x >= 0) & (near_x < pieces))
            def _():
                spread_near(2, xq, near_x)

        @pl.when(outer & (depth == 1) & (t >= pieces) & (t < 2 * pieces))
        def _():
            j = t - pieces
            send(row_piece(xq, core, j), stray_piece(1, j), tx.at[7], rx_stray.at[1, j], onward_dev)

        @pl.when(outer & (depth == 2) & (side == 0) & (t >= 2 * pieces - 2) & (t < 2 * pieces + early - 2))
        def _():
            for shift in range(2):
                j = 2 * (t - 2 * pieces + 2) + shift
                send(row_piece(w, core, j), stray_piece(2, j), tx.at[7], rx_stray.at[2, j], onward_dev)

        hop = t - pieces - early - 4

        @pl.when(relay & (hop >= 0) & (hop < early))
        def _():
            for way, chip, lone_at, x_side, here in ((0, 0, 1, 2, has_down), (1, 3, 0, 1, has_up)):
                @pl.when(here)
                def _():
                    j = hop + jnp.where(w == x_side, 0, early)
                    ref = stray_piece(way, j)
                    arrived(ref, rx_stray.at[way, j])
                    send_col(ref, late_slot(chip, core), j, 10 + way, (z, 2 * chip + lone_at))

        m = jnp.where(t < pieces + early + 1, t - pieces - 1, t - pieces - early + 5)

        @pl.when((m >= 0) & (m < 8) & ((m >= 6) == (t >= pieces + early + 1)))
        def _():
            quarter = jnp.where(m < 2, w, jnp.where(m < 4, xq, jnp.where(m < 6, yq, dq)))
            shard = 2 * quarter + m % 2
            copy = pltpu.make_async_copy(rowbuf.at[shard], stage, stage_sem.at[0])
            copy.start()
            copy.wait()

            def convert(k, carry):
                start = pl.multiple_of(k * panel_rows + shard * shard_rows, shard_rows)
                split_into(stage[k], row_lead, row_trail, start)
                return carry

            lax.fori_loop(0, kinds, convert, 0)

        lax.fori_loop(done(t - 1), done(t), quantum, 0)
        return carry

    lax.fori_loop(0, last + 3, step, 0)

    for bank in range(2):
        for k in range(perturbations):
            acc_copy(bank, k, 0).wait()

    def drain(slot, ref):
        pltpu.make_async_copy(ref, ref, tx.at[slot]).wait()

    def drain_shards(slot, count, condition):
        @pl.when(condition)
        def _():
            drain(slot, rowbuf.at[pl.ds(0, count)])

    drain(0, rowbuf.at[0])
    drain(1, rowbuf.at[0])
    drain(2, rowbuf.at[0, pl.ds(0, kinds // 2)])
    drain(3, rowbuf.at[0, pl.ds(0, kinds // 2)])
    drain(4, rowbuf.at[pl.ds(0, 4)])
    drain_shards(5, 3, has_up & (z >= w))
    drain_shards(6, 3, has_down & (z <= w))
    for count in (1, 2, 3):
        drain_shards(7, count, outer & (depth == count - 1))
        drain_shards(8, count, outer & (depth == count))
    drain_shards(9, 1, lone)
    for way, here in ((0, has_down), (1, has_up)):
        @pl.when(relay & here)
        def _():
            drain(10 + way, rowbuf.at[0, pl.ds(0, kinds // 2)])


def panels(response_coeffs, occupied_coeffs):
    perturbations, shard_rows, orbitals = response_coeffs.shape
    kinds = perturbations + 1
    pieces = kinds * CUTS
    any_space = pl.BlockSpec(memory_space=pl.ANY)
    float32, bfloat16 = jnp.float32, jnp.bfloat16
    return pl.pallas_call(
        panel_kernel,
        out_shape=(
            jax.ShapeDtypeStruct((perturbations, 8 * shard_rows, 4 * shard_rows), float32),
            jax.ShapeDtypeStruct((8, kinds, shard_rows, orbitals), float32),
            jax.ShapeDtypeStruct((5, kinds, shard_rows, orbitals), float32),
            jax.ShapeDtypeStruct((3, kinds, shard_rows, orbitals), float32),
        ),
        in_specs=[any_space] * 2,
        out_specs=(any_space,) * 4,
        scratch_shapes=[
            pltpu.VMEM((kinds * 8 * shard_rows, orbitals), bfloat16),
            pltpu.VMEM((kinds * 8 * shard_rows, orbitals), bfloat16),
            pltpu.VMEM((shard_rows, orbitals), bfloat16),
            pltpu.VMEM((shard_rows, orbitals), bfloat16),
            pltpu.VMEM((kinds, shard_rows, orbitals), float32),
            pltpu.VMEM((2, perturbations, 8 * shard_rows, shard_rows), float32),
            pltpu.SemaphoreType.DMA((8, pieces)),
            pltpu.SemaphoreType.DMA((5, pieces)),
            pltpu.SemaphoreType.DMA((3, pieces)),
            pltpu.SemaphoreType.DMA((12,)),
            pltpu.SemaphoreType.DMA((2,)),
            pltpu.SemaphoreType.DMA((2, perturbations)),
        ],
        compiler_params=pltpu.CompilerParams(
            collective_id=0, has_side_effects=True, vmem_limit_bytes=66_000_000
        ),
    )(response_coeffs, occupied_coeffs)[0]


def solution(mesh):
    fits = mesh.shape["row"] == 4 and mesh.shape["col"] == 8
    return jax.shard_map(
        panels if fits else shards,
        mesh=mesh,
        in_specs=(P(None, ("row", "col"), None), P(("row", "col"), None)),
        out_specs=P(None, "row", "col"),
        check_vma=False,
    )
```

```python
import functools

import jax
import jax.numpy as jnp
from jax import lax
from jax.experimental import pallas as pl
from jax.experimental.pallas import tpu as pltpu
from jax.sharding import PartitionSpec as P

SLICE_PAIRS = ((0, 0), (0, 1), (1, 0))


def partner(value, axis, stride):
    mask = 2**stride
    pairs = [(source, source ^ mask) for source in range(lax.axis_size(axis))]
    return lax.ppermute(value, axis, pairs)


def split_slices(values):
    leading = lax.optimization_barrier(values.astype(jnp.bfloat16))
    remainder = values - leading.astype(jnp.float32)
    trailing = lax.optimization_barrier(remainder.astype(jnp.bfloat16))
    return [leading, trailing]


def contribute(row_slices, column_slices, perturbations):
    accumulated = jnp.zeros(
        (perturbations, row_slices[0].shape[1], column_slices[0].shape[1]), jnp.float32
    )
    for left_index, right_index in SLICE_PAIRS:
        forward_term = jnp.einsum(
            "kro,co->krc",
            row_slices[left_index][:perturbations],
            column_slices[right_index][perturbations],
            preferred_element_type=jnp.float32,
        )
        mirror_term = jnp.einsum(
            "ro,kco->krc",
            row_slices[right_index][perturbations],
            column_slices[left_index][:perturbations],
            preferred_element_type=jnp.float32,
        )
        accumulated = accumulated + forward_term + mirror_term
    return accumulated


def relay_columns(stacked, perturbations):
    rows_total = lax.axis_size("row")
    columns_total = lax.axis_size("col")
    col_index = lax.axis_index("col")
    shard_rows = stacked.shape[1]
    orbitals = stacked.shape[2]
    half_rows = shard_rows // 2
    swap_bit = rows_total.bit_length() - 1
    own_first = stacked[:, :half_rows]
    partner_second = partner(stacked[:, half_rows:], "col", swap_bit)
    even_first = col_index // rows_total == 0
    leading = jnp.where(even_first, own_first, partner_second)
    trailing = jnp.where(even_first, partner_second, own_first)
    paired = jnp.concatenate([leading, trailing], axis=1)
    gathered = lax.all_gather(paired, "row", axis=1, tiled=True)
    regrouped = lax.all_to_all(gathered, "col", split_axis=1, concat_axis=1, tiled=True)
    shaped = regrouped.reshape(perturbations + 1, 2, rows_total, half_rows, orbitals)
    flipped = shaped[:, ::-1]
    ordered = jnp.where(col_index % 2 == 0, shaped, flipped)
    return jnp.swapaxes(ordered, 1, 2).reshape(
        perturbations + 1, columns_total * half_rows, orbitals
    )


def shards(response_coeffs, occupied_coeffs):
    perturbations = response_coeffs.shape[0]
    stacked = jnp.concatenate([response_coeffs, occupied_coeffs[None]], axis=0)
    column_panel = relay_columns(stacked, perturbations)
    column_slices = split_slices(column_panel)
    return contribute(
        split_slices(lax.all_gather(stacked, "col", axis=1, tiled=True)),
        column_slices,
        perturbations,
    )


CUTS = 4


def flip(value):
    return value + 1 - 2 * (value % 2)


def across(value):
    return value + 2 - 4 * (value // 2)


def panel_kernel(
    resp, occ, out, rowbuf, colbuf, straybuf,
    row_lead, row_trail, col_lead, col_trail, stage,
    rx_row, rx_col, rx_stray, tx, stage_sem,
):
    perturbations, shard_rows, orbitals = resp.shape
    kinds = perturbations + 1
    cut = shard_rows // CUTS
    pieces = kinds * CUTS
    early = pieces // 2
    panel_rows = 8 * shard_rows
    block_rows = panel_rows // 2
    row_blocks = panel_rows // block_rows

    z = lax.axis_index("row")
    planes = lax.axis_size("row")
    column = lax.axis_index("col")
    w, core = column // 2, column % 2
    xq, yq, dq = flip(w), across(w), flip(across(w))
    other = 1 - core
    x_dev, y_dev, p_dev = (z, 2 * xq + core), (z, 2 * yq + core), (z, 2 * w + other)
    up_dev, down_dev = (z + 1, column), (z - 1, column)
    has_up, has_down = z < planes - 1, z > 0
    diagonal = z == w
    match = w // 2 == core
    distance = jnp.where(z > w, z - w, w - z)

    lone = ((z > w) & (core == 1)) | ((z < w) & (core == 0))

    rising = w == 3
    outer = rising | (w == 0)
    depth = jnp.where(rising, z, planes - 1 - z)
    side = jnp.where(rising, core, other)
    lone_core = jnp.where(rising, 1, 0)
    onward_dev = (jnp.where(rising, z + 1, z - 1), column)
    inbound = outer & (depth > 0)
    onward = outer & (depth < planes - 1)
    relay = (w == 1) | (w == 2)

    ending = ((z == planes - 1) | (z == 0)) & jnp.logical_not(diagonal)
    scale = CUTS // 4
    hop = scale

    barrier = pltpu.get_barrier_semaphore()

    def greet(device):
        pl.semaphore_signal(barrier, inc=1, device_id=device, device_id_type=pl.DeviceIdType.MESH)

    for device in (x_dev, y_dev, p_dev, (z, 2 * xq + other), (z, 2 * yq + other)):
        greet(device)

    @pl.when(has_up)
    def _():
        greet(up_dev)

    @pl.when(has_down)
    def _():
        greet(down_dev)

    pl.semaphore_wait(barrier, 5 + jnp.where(has_up, 1, 0) + jnp.where(has_down, 1, 0))

    def rows_at(j):
        return pl.ds(pl.multiple_of((j % CUTS) * cut, cut), cut)

    def row_piece(quarter, lane, j):
        return rowbuf.at[2 * quarter + lane, j // CUTS, rows_at(j)]

    def col_piece(slot, j):
        return colbuf.at[slot, j // CUTS, rows_at(j)]

    def stray_piece(q, j):
        return straybuf.at[q, j // CUTS, rows_at(j)]

    def send(source, target, send_sem, recv_sem, device):
        pltpu.make_async_remote_copy(
            src_ref=source, dst_ref=target, send_sem=send_sem, recv_sem=recv_sem,
            device_id=device, device_id_type=pl.DeviceIdType.MESH,
        ).start()

    def send_row(quarter, lane, j, slot, device):
        ref = row_piece(quarter, lane, j)
        send(ref, ref, tx.at[slot], rx_row.at[2 * quarter + lane, j], device)

    def arrived(ref, sem):
        pltpu.make_async_copy(ref, ref, sem).wait()

    def wait_row(quarter, lane, j):
        arrived(row_piece(quarter, lane, j), rx_row.at[2 * quarter + lane, j])

    def wait_col(slot, j):
        arrived(col_piece(slot, j), rx_col.at[slot, j])

    def send_col(source, slot, j, way, device):
        send(source, col_piece(slot, j), tx.at[way], rx_col.at[slot, j], device)

    def held(k):
        return out.at[0, pl.ds(k * shard_rows, shard_rows)]

    own = [occ] + [resp.at[k] for k in range(perturbations)]
    loads = [pltpu.make_async_copy(own[k], held(k), stage_sem.at[k]) for k in range(kinds)]
    keeps = [pltpu.make_async_copy(held(k), rowbuf.at[2 * w + core, k], stage_sem.at[k]) for k in range(kinds)]
    for load in loads:
        load.start()

    def launch(source, j):
        for slot, device in ((0, x_dev), (1, y_dev), (4, p_dev)):
            send(source, row_piece(w, core, j), tx.at[slot], rx_row.at[2 * w + core, j], device)

        @pl.when(diagonal & match & has_up)
        def _():
            send_col(source, 0, j, 5, up_dev)

        @pl.when(diagonal & match & has_down)
        def _():
            send_col(source, 0, j, 6, down_dev)

        @pl.when(outer & ((depth == 0) | ((depth == 2) & (side == 1))))
        def _():
            send(source, stray_piece(depth, j), tx.at[7], rx_stray.at[depth, j], onward_dev)

    def launch_occ(j, carry):
        launch(occ.at[rows_at(j)], j)
        return carry

    def launch_resp(j, carry):
        launch(resp.at[j // CUTS - 1, rows_at(j)], j)
        return carry

    lax.fori_loop(0, CUTS, launch_occ, 0)
    lax.fori_loop(CUTS, pieces, launch_resp, 0)
    for load, keep in zip(loads, keeps):
        load.wait()
        keep.start()
    for keep in keeps:
        keep.wait()

    first = jnp.where(match, w, yq)
    second = flip(first)
    early_lane = jnp.where(lone, 1 - w % 2, core)

    def order(i):
        double_first = (i == 0) | (i == 3)
        quarter = jnp.where(lone, jnp.where(i < 2, first, second), jnp.where(double_first, first, second))
        lone_lane = jnp.where(i < 2, core, early_lane)
        lone_lane = jnp.where(i % 2 == 0, lone_lane, 1 - lone_lane)
        lane = jnp.where(lone, lone_lane, jnp.where(i < 2, core, other))
        return quarter, lane

    def chain_order(b, double):
        quarter = jnp.where(b == 0, first, jnp.where(double, second, jnp.where(b == 1, first, across(first))))
        lane = jnp.where(jnp.where(double, b == 2, b == 1), other, core)
        return quarter, lane

    def chain_slot(b, double):
        return jnp.where(double | (b < 2), b, 4)

    def emit_own(p, carry):
        b, j = p // pieces, p % pieces

        @pl.when(has_up)
        def _():
            quarter, lane = chain_order(b, core == 0)
            send_col(row_piece(quarter, lane, j), chain_slot(b, core == 0), j, 5, up_dev)

        @pl.when(has_down)
        def _():
            quarter, lane = chain_order(b, core == 1)
            send_col(row_piece(quarter, lane, j), chain_slot(b, core == 1), j, 6, down_dev)

        return carry

    def pass_on(p, carry):
        b, j = p // pieces, p % pieces
        slot = chain_slot(b, jnp.logical_not(lone))
        wait_col(slot, j)
        source = col_piece(slot, j)

        @pl.when(has_up & (z > w))
        def _():
            send_col(source, slot, j, 5, up_dev)

        @pl.when(has_down & (z < w))
        def _():
            send_col(source, slot, j, 6, down_dev)

        @pl.when(slot == 4)
        def _():
            send_col(source, 3, j, 9, p_dev)

        return carry

    def clip(value, most):
        return jnp.minimum(jnp.maximum(value, 0), most)

    last = 3 * pieces

    def sent(t):
        slow = t + 1 + jnp.maximum(t - pieces - early, 0)
        return clip(jnp.where(match, pieces + t + 1, slow), last)

    def received(t):
        return clip(t - hop * (distance - 1) + 1, last)

    def stray_order(i):
        b = i // pieces
        return jnp.where((depth == 3) & (side == 1), (b + 2) % 3, b)

    def stray_received(t):
        near_end = 2 * (pieces + scale)
        late = jnp.where(t < near_end, t - (3 * hop + 2) + (1 if scale == 1 else 0), t - 2 * scale + 1)
        farthest = jnp.where(side == 1, t, late)
        return clip(jnp.where(depth == 1, t + 1, jnp.where(depth == 2, t - hop, farthest)), depth * pieces)

    def take_stray(i, carry):
        q, j = stray_order(i), i % pieces
        ref = stray_piece(q, j)
        arrived(ref, rx_stray.at[q, j])

        @pl.when(onward)
        def _():
            send(ref, ref, tx.at[7], rx_stray.at[q, j], onward_dev)

        return carry

    def late_slot(chip, lane):
        return 2 + jnp.where(lane == 1 - chip % 2, 0, 1)

    through = jnp.where(rising, 0, 1)

    def spread_far(j):
        chip = jnp.where(j < early, xq, yq)
        send(stray_piece(0, j), stray_piece(through, j), tx.at[8], rx_stray.at[through, j], (z, 2 * chip + core))

    def spread_near(q, chip, j):
        send_col(stray_piece(q, j), late_slot(chip, core), j, 8, (z, 2 * chip + lone_core))

    def split_into(value, lead, trail, start):
        leading = value.astype(jnp.bfloat16)
        lead[pl.ds(start, shard_rows), :] = leading
        trail[pl.ds(start, shard_rows), :] = (value - leading.astype(jnp.float32)).astype(jnp.bfloat16)

    opening_units = 1 + perturbations * row_blocks
    closing_units = 1 + row_blocks
    half_units = 1 + 3 * perturbations
    halves = 4
    own_block = w // 2

    due = []
    for start in (19.6, 26.7, 29.9, 33.1):
        due += [start + 0.32 * unit for unit in range(half_units)]
    due += [36.4 + 0.3 * unit for unit in range(2 * opening_units)]
    shown = [40.6, 41.6, 44.4, 45.4, 48, 48]
    hidden = [44.4, 45.4, 49, 49, 49, 49]
    due_early = due + [start + 0.3 * unit for start in shown for unit in range(closing_units)]
    due_late = due + [start + 0.3 * unit for start in hidden for unit in range(closing_units)]
    lag = jnp.where(diagonal, 0, jnp.maximum(hop * (distance - 1), jnp.where(lone, scale, 0)))

    def done(t):
        count = 0
        for soon, later in zip(due_early, due_late):
            soon, later = min(int(soon * scale), last), int(later * scale)
            time = soon if soon == later else jnp.where(ending, soon, later)
            count = count + jnp.where(t - lag >= time, 1, 0)
        return jnp.where(t >= last + 3 * scale - 1, len(due_early), count)

    def block_of(ref, kind, block):
        return ref[pl.ds(pl.multiple_of(kind * panel_rows + block * block_rows, block_rows), block_rows), :]

    def product(left, right):
        return lax.dot_general(left, right, (((1,), (1,)), ((), ())), preferred_element_type=jnp.float32)

    def total(kind, block):
        lead, trail = block_of(row_lead, kind, block), block_of(row_trail, kind, block)
        value = product(lead, col_lead[...])
        value += product(lead, col_trail[...])
        value += product(trail, col_lead[...])
        return value

    def target(block):
        return pl.ds(pl.multiple_of(block * block_rows, block_rows), block_rows)

    def quantum(g, carry):
        half, x = g // half_units, g % half_units
        y = x - 1 - perturbations
        h = g - halves * half_units
        early_work = h < 0
        e = h - 2 * opening_units
        slot = jnp.where(early_work, half // 2, jnp.where(e < 0, h // opening_units, (e // closing_units) % 2) + 2)
        closing = e % closing_units
        begin = h % opening_units
        opening = jnp.where(early_work, y < 0, e < 0)
        fetching = jnp.where(early_work, (x == 0) | ((y >= 0) & (y % 2 == 0)), jnp.where(e < 0, begin == 0, closing == 0))
        early_k = jnp.where(y < 0, x - 1, y // 2)
        k = jnp.where(early_work, early_k, jnp.where(e < 0, (begin - 1) // row_blocks, e // (2 * closing_units)))
        early_block = jnp.where(half % 2 == 0, own_block, 1 - own_block)
        block = jnp.where(early_work, early_block, jnp.where(e < 0, (begin - 1) % row_blocks, closing - 1))
        kind = jnp.where(opening, 0, k + 1)
        quarter, lane = order(slot)
        place = pl.ds(pl.multiple_of((2 * (quarter % 2) + lane) * shard_rows, shard_rows), shard_rows)

        @pl.when(fetching)
        def _():
            @pl.when((z != w) & ((slot == 3) | (lone & (slot == 2))))
            def _():
                def late_wait(j, carry):
                    wait_col(slot, kind * CUTS + j)
                    return carry

                lax.fori_loop(0, CUTS, late_wait, 0)

            def fetch(kind, way):
                @pl.when(diagonal)
                def _():
                    pltpu.make_async_copy(rowbuf.at[2 * quarter + lane, kind], stage.at[way], stage_sem.at[way]).start()

                @pl.when(z != w)
                def _():
                    pltpu.make_async_copy(colbuf.at[slot, kind], stage.at[way], stage_sem.at[way]).start()

            way = jnp.where(early_work, kind % 2, 0)

            @pl.when((kind == 0) | jnp.logical_not(early_work))
            def _():
                fetch(kind, way)

            @pl.when(early_work & (kind < perturbations))
            def _():
                fetch(kind + 1, 1 - way)

            arrived(stage.at[way], stage_sem.at[way])
            split_into(stage[way], col_lead, col_trail, 0)

        @pl.when(opening & jnp.logical_not(fetching))
        def _():
            out[k, target(block), place] = total(k + 1, block)

        @pl.when(jnp.logical_not(opening | fetching))
        def _():
            out[k, target(block), place] += total(0, block)

        return carry

    def step(t, carry):
        @pl.when(t < pieces)
        def _():
            wait_row(xq, core, t)
            send_row(xq, core, t, 4, p_dev)
            wait_row(yq, core, t)
            send_row(yq, core, t, 4, p_dev)
            wait_row(w, other, t)

            @pl.when(t < early)
            def _():
                send_row(yq, core, t, 2, x_dev)

            @pl.when(t >= early)
            def _():
                send_row(xq, core, t, 3, y_dev)

        @pl.when((t >= 1) & (t < pieces + 1))
        def _():
            wait_row(xq, other, t - 1)
            wait_row(yq, other, t - 1)

        @pl.when((t >= pieces) & (t < pieces + early))
        def _():
            for shift in (0, early):
                wait_row(dq, core, t - pieces + shift)
                send_row(dq, core, t - pieces + shift, 4, p_dev)

        @pl.when((t >= pieces + 1) & (t < pieces + early + 1))
        def _():
            for shift in (0, early):
                wait_row(dq, other, t - pieces - 1 + shift)

        @pl.when(diagonal)
        def _():
            lax.fori_loop(sent(t - 1), sent(t), emit_own, 0)

        @pl.when(z != w)
        def _():
            lax.fori_loop(received(t - 1), received(t), pass_on, 0)

        @pl.when(inbound)
        def _():
            lax.fori_loop(stray_received(t - 1), stray_received(t), take_stray, 0)
            far = t - pieces - 2
            near = t - pieces - early - 2
            near_x = jnp.where(side == 0, t - 2 * (pieces + scale), near)
            near_y = jnp.where(side == 1, t - 2 * pieces - 2, near)

            @pl.when((far >= 0) & (far < jnp.where(side == 0, early, pieces)))
            def _():
                spread_far(far)

            @pl.when((side == 0) & (far >= 0) & (far < early))
            def _():
                spread_far(far + early)

            @pl.when((depth > 1) & (near_y >= 0) & (near_y < pieces))
            def _():
                spread_near(1, yq, near_y)

            @pl.when((depth > 2) & (near_x >= 0) & (near_x < pieces))
            def _():
                spread_near(2, xq, near_x)

        @pl.when(outer & (depth == 1) & (t >= pieces) & (t < 2 * pieces))
        def _():
            j = t - pieces
            send(row_piece(xq, core, j), stray_piece(1, j), tx.at[7], rx_stray.at[1, j], onward_dev)

        @pl.when(outer & (depth == 2) & (side == 0) & (t >= 2 * (pieces - scale)) & (t < 2 * (pieces - scale) + early))
        def _():
            for shift in range(2):
                j = 2 * (t - 2 * (pieces - scale)) + shift
                send(row_piece(w, core, j), stray_piece(2, j), tx.at[7], rx_stray.at[2, j], onward_dev)

        turn = t - pieces - early - 2 * scale - 2

        @pl.when(relay & (turn >= 0) & (turn < early))
        def _():
            for way, chip, lone_at, x_side, here in ((0, 0, 1, 2, has_down), (1, 3, 0, 1, has_up)):
                @pl.when(here)
                def _():
                    j = turn + jnp.where(w == x_side, 0, early)
                    ref = stray_piece(way, j)
                    arrived(ref, rx_stray.at[way, j])
                    send_col(ref, late_slot(chip, core), j, 10 + way, (z, 2 * chip + lone_at))

        def load(task):
            m, kind = task // kinds, task % kinds
            quarter = jnp.where(m < 2, w, jnp.where(m < 4, xq, jnp.where(m < 6, yq, dq)))
            shard, way = 2 * quarter + m % 2, task % 2
            copy = pltpu.make_async_copy(rowbuf.at[shard, kind], stage.at[way], stage_sem.at[way])
            return copy, way, kind * panel_rows + shard * shard_rows

        def convert(task, carry):
            copy, way, start = load(task)

            @pl.when((task == 0) | (task == 6 * kinds))
            def _():
                copy.start()

            @pl.when((task + 1 != 6 * kinds) & (task + 1 < 8 * kinds))
            def _():
                load(task + 1)[0].start()

            copy.wait()
            split_into(stage[way], row_lead, row_trail, pl.multiple_of(start, shard_rows))
            return carry

        def converted(t):
            near_tasks = clip((t - pieces) * 8 // scale, 6 * kinds)
            return near_tasks + clip((t - pieces - early) * 4 // scale, 2 * kinds)

        lax.fori_loop(converted(t - 1), converted(t), convert, 0)
        ready = done(t)
        lax.fori_loop(carry, ready, quantum, 0)
        carry = ready
        return carry

    lax.fori_loop(0, last + 3 * scale, step, 0)

    def drain(slot, ref):
        pltpu.make_async_copy(ref, ref, tx.at[slot]).wait()

    def drain_shards(slot, count, condition):
        @pl.when(condition)
        def _():
            drain(slot, rowbuf.at[pl.ds(0, count)])

    drain(0, rowbuf.at[0])
    drain(1, rowbuf.at[0])
    drain(2, rowbuf.at[0, pl.ds(0, kinds // 2)])
    drain(3, rowbuf.at[0, pl.ds(0, kinds // 2)])
    drain(4, rowbuf.at[pl.ds(0, 4)])
    drain_shards(5, 3, has_up & (z >= w))
    drain_shards(6, 3, has_down & (z <= w))
    for count in (1, 2, 3):
        drain_shards(7, count, outer & (depth == count - 1))
        drain_shards(8, count, outer & (depth == count))
    drain_shards(9, 1, lone)
    for way, here in ((0, has_down), (1, has_up)):
        @pl.when(relay & here)
        def _():
            drain(10 + way, rowbuf.at[0, pl.ds(0, kinds // 2)])


def panels(response_coeffs, occupied_coeffs):
    perturbations, shard_rows, orbitals = response_coeffs.shape
    kinds = perturbations + 1
    pieces = kinds * CUTS
    any_space = pl.BlockSpec(memory_space=pl.ANY)
    float32, bfloat16 = jnp.float32, jnp.bfloat16
    return pl.pallas_call(
        panel_kernel,
        out_shape=(
            pltpu.VMEM((perturbations, 8 * shard_rows, 4 * shard_rows), float32),
            jax.ShapeDtypeStruct((8, kinds, shard_rows, orbitals), float32),
            jax.ShapeDtypeStruct((5, kinds, shard_rows, orbitals), float32),
            jax.ShapeDtypeStruct((3, kinds, shard_rows, orbitals), float32),
        ),
        in_specs=[any_space] * 2,
        out_specs=(pl.BlockSpec(memory_space=pltpu.VMEM),) + (any_space,) * 3,
        scratch_shapes=[
            pltpu.VMEM((kinds * 8 * shard_rows, orbitals), bfloat16),
            pltpu.VMEM((kinds * 8 * shard_rows, orbitals), bfloat16),
            pltpu.VMEM((shard_rows, orbitals), bfloat16),
            pltpu.VMEM((shard_rows, orbitals), bfloat16),
            pltpu.VMEM((2, shard_rows, orbitals), float32),
            pltpu.SemaphoreType.DMA((8, pieces)),
            pltpu.SemaphoreType.DMA((5, pieces)),
            pltpu.SemaphoreType.DMA((3, pieces)),
            pltpu.SemaphoreType.DMA((12,)),
            pltpu.SemaphoreType.DMA((kinds,)),
        ],
        compiler_params=pltpu.CompilerParams(
            collective_id=0, has_side_effects=True, vmem_limit_bytes=41_300_000
        ),
    )(response_coeffs, occupied_coeffs)[0]


def store_kernel(held, out, sem):
    copies = [pltpu.make_async_copy(held.at[k], out.at[k], sem.at[k]) for k in range(held.shape[0])]
    for copy in copies:
        copy.start()
    for copy in copies:
        copy.wait()


def store(held):
    return pl.pallas_call(
        store_kernel,
        out_shape=jax.ShapeDtypeStruct(held.shape, held.dtype),
        in_specs=[pl.BlockSpec(memory_space=pltpu.VMEM)],
        out_specs=pl.BlockSpec(memory_space=pl.ANY),
        scratch_shapes=[pltpu.SemaphoreType.DMA((held.shape[0],))],
        compiler_params=pltpu.CompilerParams(vmem_limit_bytes=1_000_000),
    )(held)


def solution(mesh):
    fits = mesh.shape["row"] == 4 and mesh.shape["col"] == 8
    return jax.shard_map(
        (lambda *args: store(panels(*args))) if fits else shards,
        mesh=mesh,
        in_specs=(P(None, ("row", "col"), None), P(("row", "col"), None)),
        out_specs=P(None, "row", "col"),
        check_vma=False,
    )
```

```python
import functools

import jax
import jax.numpy as jnp
from jax import lax
from jax.experimental import pallas as pl
from jax.experimental.pallas import tpu as pltpu
from jax.sharding import PartitionSpec as P

SLICE_PAIRS = ((0, 0), (0, 1), (1, 0))


def partner(value, axis, stride):
    mask = 2**stride
    pairs = [(source, source ^ mask) for source in range(lax.axis_size(axis))]
    return lax.ppermute(value, axis, pairs)


def split_slices(values):
    leading = lax.optimization_barrier(values.astype(jnp.bfloat16))
    remainder = values - leading.astype(jnp.float32)
    trailing = lax.optimization_barrier(remainder.astype(jnp.bfloat16))
    return [leading, trailing]


def contribute(row_slices, column_slices, perturbations):
    accumulated = jnp.zeros(
        (perturbations, row_slices[0].shape[1], column_slices[0].shape[1]), jnp.float32
    )
    for left_index, right_index in SLICE_PAIRS:
        forward_term = jnp.einsum(
            "kro,co->krc",
            row_slices[left_index][:perturbations],
            column_slices[right_index][perturbations],
            preferred_element_type=jnp.float32,
        )
        mirror_term = jnp.einsum(
            "ro,kco->krc",
            row_slices[right_index][perturbations],
            column_slices[left_index][:perturbations],
            preferred_element_type=jnp.float32,
        )
        accumulated = accumulated + forward_term + mirror_term
    return accumulated


def relay_columns(stacked, perturbations):
    rows_total = lax.axis_size("row")
    columns_total = lax.axis_size("col")
    col_index = lax.axis_index("col")
    shard_rows = stacked.shape[1]
    orbitals = stacked.shape[2]
    half_rows = shard_rows // 2
    swap_bit = rows_total.bit_length() - 1
    own_first = stacked[:, :half_rows]
    partner_second = partner(stacked[:, half_rows:], "col", swap_bit)
    even_first = col_index // rows_total == 0
    leading = jnp.where(even_first, own_first, partner_second)
    trailing = jnp.where(even_first, partner_second, own_first)
    paired = jnp.concatenate([leading, trailing], axis=1)
    gathered = lax.all_gather(paired, "row", axis=1, tiled=True)
    regrouped = lax.all_to_all(gathered, "col", split_axis=1, concat_axis=1, tiled=True)
    shaped = regrouped.reshape(perturbations + 1, 2, rows_total, half_rows, orbitals)
    flipped = shaped[:, ::-1]
    ordered = jnp.where(col_index % 2 == 0, shaped, flipped)
    return jnp.swapaxes(ordered, 1, 2).reshape(
        perturbations + 1, columns_total * half_rows, orbitals
    )


def shards(response_coeffs, occupied_coeffs):
    perturbations = response_coeffs.shape[0]
    stacked = jnp.concatenate([response_coeffs, occupied_coeffs[None]], axis=0)
    column_panel = relay_columns(stacked, perturbations)
    column_slices = split_slices(column_panel)
    return contribute(
        split_slices(lax.all_gather(stacked, "col", axis=1, tiled=True)),
        column_slices,
        perturbations,
    )


CUTS = 4
STORES = 4


def flip(value):
    return value + 1 - 2 * (value % 2)


def across(value):
    return value + 2 - 4 * (value // 2)


def panel_kernel(
    resp, occ, out, rowbuf, colbuf, straybuf,
    row_lead, row_trail, col_lead, col_trail, stage,
    rx_row, rx_col, rx_stray, tx, stage_sem,
):
    perturbations, shard_rows, orbitals = resp.shape
    kinds = perturbations + 1
    cut = shard_rows // CUTS
    pieces = kinds * CUTS
    early = pieces // 2
    panel_rows = 8 * shard_rows
    block_rows = panel_rows // 2
    row_blocks = panel_rows // block_rows

    z = lax.axis_index("row")
    planes = lax.axis_size("row")
    column = lax.axis_index("col")
    w, core = column // 2, column % 2
    xq, yq, dq = flip(w), across(w), flip(across(w))
    other = 1 - core
    x_dev, y_dev, p_dev = (z, 2 * xq + core), (z, 2 * yq + core), (z, 2 * w + other)
    up_dev, down_dev = (z + 1, column), (z - 1, column)
    has_up, has_down = z < planes - 1, z > 0
    diagonal = z == w
    match = w // 2 == core
    distance = jnp.where(z > w, z - w, w - z)

    lone = ((z > w) & (core == 1)) | ((z < w) & (core == 0))

    rising = w == 3
    outer = rising | (w == 0)
    depth = jnp.where(rising, z, planes - 1 - z)
    side = jnp.where(rising, core, other)
    lone_core = jnp.where(rising, 1, 0)
    onward_dev = (jnp.where(rising, z + 1, z - 1), column)
    inbound = outer & (depth > 0)
    onward = outer & (depth < planes - 1)
    relay = (w == 1) | (w == 2)

    ending = ((z == planes - 1) | (z == 0)) & jnp.logical_not(diagonal)
    scale = CUTS // 4
    hop = scale

    barrier = pltpu.get_barrier_semaphore()

    def greet(device):
        pl.semaphore_signal(barrier, inc=1, device_id=device, device_id_type=pl.DeviceIdType.MESH)

    for device in (x_dev, y_dev, p_dev, (z, 2 * xq + other), (z, 2 * yq + other)):
        greet(device)

    @pl.when(has_up)
    def _():
        greet(up_dev)

    @pl.when(has_down)
    def _():
        greet(down_dev)

    pl.semaphore_wait(barrier, 5 + jnp.where(has_up, 1, 0) + jnp.where(has_down, 1, 0))

    def rows_at(j):
        return pl.ds(pl.multiple_of((j % CUTS) * cut, cut), cut)

    def row_piece(quarter, lane, j):
        return rowbuf.at[2 * quarter + lane, j // CUTS, rows_at(j)]

    def col_piece(slot, j):
        return colbuf.at[slot, j // CUTS, rows_at(j)]

    def stray_piece(q, j):
        return straybuf.at[q, j // CUTS, rows_at(j)]

    def send(source, target, send_sem, recv_sem, device):
        pltpu.make_async_remote_copy(
            src_ref=source, dst_ref=target, send_sem=send_sem, recv_sem=recv_sem,
            device_id=device, device_id_type=pl.DeviceIdType.MESH,
        ).start()

    def send_row(quarter, lane, j, slot, device):
        ref = row_piece(quarter, lane, j)
        send(ref, ref, tx.at[slot], rx_row.at[2 * quarter + lane, j], device)

    def arrived(ref, sem):
        pltpu.make_async_copy(ref, ref, sem).wait()

    def wait_row(quarter, lane, j):
        arrived(row_piece(quarter, lane, j), rx_row.at[2 * quarter + lane, j])

    def wait_col(slot, j):
        arrived(col_piece(slot, j), rx_col.at[slot, j])

    def send_col(source, slot, j, way, device):
        send(source, col_piece(slot, j), tx.at[way], rx_col.at[slot, j], device)

    def held(k):
        return out.at[0, pl.ds(k * shard_rows, shard_rows)]

    own = [occ] + [resp.at[k] for k in range(perturbations)]
    loads = [pltpu.make_async_copy(own[k], held(k), stage_sem.at[k]) for k in range(kinds)]
    keeps = [pltpu.make_async_copy(held(k), rowbuf.at[2 * w + core, k], stage_sem.at[k]) for k in range(kinds)]
    for load in loads:
        load.start()

    def launch(source, j):
        for slot, device in ((0, x_dev), (1, y_dev), (4, p_dev)):
            send(source, row_piece(w, core, j), tx.at[slot], rx_row.at[2 * w + core, j], device)

        @pl.when(diagonal & match & has_up)
        def _():
            send_col(source, 0, j, 5, up_dev)

        @pl.when(diagonal & match & has_down)
        def _():
            send_col(source, 0, j, 6, down_dev)

        @pl.when(outer & ((depth == 0) | ((depth == 2) & (side == 1))))
        def _():
            send(source, stray_piece(depth, j), tx.at[7], rx_stray.at[depth, j], onward_dev)

    def launch_occ(j, carry):
        launch(occ.at[rows_at(j)], j)
        return carry

    def launch_resp(j, carry):
        launch(resp.at[j // CUTS - 1, rows_at(j)], j)
        return carry

    lax.fori_loop(0, CUTS, launch_occ, 0)
    lax.fori_loop(CUTS, pieces, launch_resp, 0)
    for load, keep in zip(loads, keeps):
        load.wait()
        keep.start()
    for keep in keeps:
        keep.wait()

    first = jnp.where(match, w, yq)
    second = flip(first)
    early_lane = jnp.where(lone, 1 - w % 2, core)

    def order(i):
        double_first = (i == 0) | (i == 3)
        quarter = jnp.where(lone, jnp.where(i < 2, first, second), jnp.where(double_first, first, second))
        lone_lane = jnp.where(i < 2, core, early_lane)
        lone_lane = jnp.where(i % 2 == 0, lone_lane, 1 - lone_lane)
        lane = jnp.where(lone, lone_lane, jnp.where(i < 2, core, other))
        return quarter, lane

    def chain_order(b, double):
        quarter = jnp.where(b == 0, first, jnp.where(double, second, jnp.where(b == 1, first, across(first))))
        lane = jnp.where(jnp.where(double, b == 2, b == 1), other, core)
        return quarter, lane

    def chain_slot(b, double):
        return jnp.where(double | (b < 2), b, 4)

    def emit_own(p, carry):
        b, j = p // pieces, p % pieces

        @pl.when(has_up)
        def _():
            quarter, lane = chain_order(b, core == 0)
            send_col(row_piece(quarter, lane, j), chain_slot(b, core == 0), j, 5, up_dev)

        @pl.when(has_down)
        def _():
            quarter, lane = chain_order(b, core == 1)
            send_col(row_piece(quarter, lane, j), chain_slot(b, core == 1), j, 6, down_dev)

        return carry

    def pass_on(p, carry):
        b, j = p // pieces, p % pieces
        slot = chain_slot(b, jnp.logical_not(lone))
        wait_col(slot, j)
        source = col_piece(slot, j)

        @pl.when(has_up & (z > w))
        def _():
            send_col(source, slot, j, 5, up_dev)

        @pl.when(has_down & (z < w))
        def _():
            send_col(source, slot, j, 6, down_dev)

        @pl.when(slot == 4)
        def _():
            send_col(source, 3, j, 9, p_dev)

        return carry

    def clip(value, most):
        return jnp.minimum(jnp.maximum(value, 0), most)

    last = 3 * pieces

    def sent(t):
        slow = t + 1 + jnp.maximum(t - pieces - early, 0)
        return clip(jnp.where(match, pieces + t + 1, slow), last)

    def received(t):
        return clip(t - hop * (distance - 1) + 1, last)

    def stray_order(i):
        b = i // pieces
        return jnp.where((depth == 3) & (side == 1), (b + 2) % 3, b)

    def stray_received(t):
        near_end = 2 * (pieces + scale)
        late = jnp.where(t < near_end, t - (3 * hop + 2) + (1 if scale == 1 else 0), t - 2 * scale + 1)
        farthest = jnp.where(side == 1, t, late)
        return clip(jnp.where(depth == 1, t + 1, jnp.where(depth == 2, t - hop, farthest)), depth * pieces)

    def take_stray(i, carry):
        q, j = stray_order(i), i % pieces
        ref = stray_piece(q, j)
        arrived(ref, rx_stray.at[q, j])

        @pl.when(onward)
        def _():
            send(ref, ref, tx.at[7], rx_stray.at[q, j], onward_dev)

        return carry

    def late_slot(chip, lane):
        return 2 + jnp.where(lane == 1 - chip % 2, 0, 1)

    through = jnp.where(rising, 0, 1)

    def spread_far(j):
        chip = jnp.where(j < early, xq, yq)
        send(stray_piece(0, j), stray_piece(through, j), tx.at[8], rx_stray.at[through, j], (z, 2 * chip + core))

    def spread_near(q, chip, j):
        send_col(stray_piece(q, j), late_slot(chip, core), j, 8, (z, 2 * chip + lone_core))

    def split_into(value, lead, trail, start):
        leading = value.astype(jnp.bfloat16)
        lead[pl.ds(start, shard_rows), :] = leading
        trail[pl.ds(start, shard_rows), :] = (value - leading.astype(jnp.float32)).astype(jnp.bfloat16)

    opening_units = 1 + perturbations * row_blocks
    closing_units = 1 + row_blocks
    half_units = 1 + 3 * perturbations
    halves = 4
    own_block = w // 2

    due = []
    for start in (19.6, 26.7, 29.9, 33.1):
        due += [start + 0.32 * unit for unit in range(half_units)]
    due += [36.4 + 0.3 * unit for unit in range(2 * opening_units)]
    shown = [40.6, 41.6, 44.4, 45.4, 48, 48]
    hidden = [42.5, 44, 46, 47.5, 49, 49]
    due_early = due + [start + 0.3 * unit for start in shown for unit in range(closing_units)]
    due_late = due + [start + 0.3 * unit for start in hidden for unit in range(closing_units)]
    lag = jnp.where(diagonal, 0, jnp.maximum(hop * (distance - 1), jnp.where(lone, scale, 0)))

    def done(t):
        count = 0
        for soon, later in zip(due_early, due_late):
            soon, later = min(int(soon * scale), last), int(later * scale)
            time = soon if soon == later else jnp.where(ending, soon, later)
            count = count + jnp.where(t - lag >= time, 1, 0)
        return jnp.where(t >= last + 3 * scale - 1, len(due_early), count)

    def block_of(ref, kind, block):
        return ref[pl.ds(pl.multiple_of(kind * panel_rows + block * block_rows, block_rows), block_rows), :]

    def product(left, right):
        return lax.dot_general(left, right, (((1,), (1,)), ((), ())), preferred_element_type=jnp.float32)

    def total(kind, block):
        lead, trail = block_of(row_lead, kind, block), block_of(row_trail, kind, block)
        value = product(lead, col_lead[...])
        value += product(lead, col_trail[...])
        value += product(trail, col_lead[...])
        return value

    def target(block):
        return pl.ds(pl.multiple_of(block * block_rows, block_rows), block_rows)

    def quantum(g, carry):
        half, x = g // half_units, g % half_units
        y = x - 1 - perturbations
        h = g - halves * half_units
        early_work = h < 0
        e = h - 2 * opening_units
        slot = jnp.where(early_work, half // 2, jnp.where(e < 0, h // opening_units, (e // closing_units) % 2) + 2)
        closing = e % closing_units
        begin = h % opening_units
        opening = jnp.where(early_work, y < 0, e < 0)
        fetching = jnp.where(early_work, (x == 0) | ((y >= 0) & (y % 2 == 0)), jnp.where(e < 0, begin == 0, closing == 0))
        early_k = jnp.where(y < 0, x - 1, y // 2)
        k = jnp.where(early_work, early_k, jnp.where(e < 0, (begin - 1) // row_blocks, e // (2 * closing_units)))
        early_block = jnp.where(half % 2 == 0, own_block, 1 - own_block)
        block = jnp.where(early_work, early_block, jnp.where(e < 0, (begin - 1) % row_blocks, closing - 1))
        kind = jnp.where(opening, 0, k + 1)
        quarter, lane = order(slot)
        place = pl.ds(pl.multiple_of((2 * (quarter % 2) + lane) * shard_rows, shard_rows), shard_rows)

        @pl.when(fetching)
        def _():
            @pl.when((z != w) & ((slot == 3) | (lone & (slot == 2))))
            def _():
                def late_wait(j, carry):
                    wait_col(slot, kind * CUTS + j)
                    return carry

                lax.fori_loop(0, CUTS, late_wait, 0)

            def fetch(slot, kind, way):
                quarter, lane = order(slot)

                @pl.when(diagonal)
                def _():
                    pltpu.make_async_copy(rowbuf.at[2 * quarter + lane, kind], stage.at[way], stage_sem.at[way]).start()

                @pl.when(z != w)
                def _():
                    pltpu.make_async_copy(colbuf.at[slot, kind], stage.at[way], stage_sem.at[way]).start()

            way = jnp.where(early_work, kind % 2, slot % 2)
            begins = jnp.logical_not(diagonal) | ((slot == 2) & (kind == 0))
            goes_on = diagonal & ((slot == 2) | (kind < perturbations))
            next_slot = jnp.where(early_work, slot, 5 - slot)
            next_kind = jnp.where(early_work | (slot == 3), kind + 1, kind)

            @pl.when(jnp.where(early_work, kind == 0, begins))
            def _():
                fetch(slot, kind, way)

            @pl.when(jnp.where(early_work, kind < perturbations, goes_on))
            def _():
                fetch(next_slot, next_kind, 1 - way)

            arrived(stage.at[way], stage_sem.at[way])
            split_into(stage[way], col_lead, col_trail, 0)

        @pl.when(opening & jnp.logical_not(fetching))
        def _():
            out[k, target(block), place] = total(k + 1, block)

        @pl.when(jnp.logical_not(opening | fetching))
        def _():
            out[k, target(block), place] += total(0, block)

        return carry

    def step(t, carry):
        @pl.when(t < pieces)
        def _():
            wait_row(xq, core, t)
            send_row(xq, core, t, 4, p_dev)
            wait_row(yq, core, t)
            send_row(yq, core, t, 4, p_dev)
            wait_row(w, other, t)

            @pl.when(t < early)
            def _():
                send_row(yq, core, t, 2, x_dev)

            @pl.when(t >= early)
            def _():
                send_row(xq, core, t, 3, y_dev)

        @pl.when((t >= 1) & (t < pieces + 1))
        def _():
            wait_row(xq, other, t - 1)
            wait_row(yq, other, t - 1)

        @pl.when((t >= pieces) & (t < pieces + early))
        def _():
            for shift in (0, early):
                wait_row(dq, core, t - pieces + shift)
                send_row(dq, core, t - pieces + shift, 4, p_dev)

        @pl.when((t >= pieces + 1) & (t < pieces + early + 1))
        def _():
            for shift in (0, early):
                wait_row(dq, other, t - pieces - 1 + shift)

        @pl.when(diagonal)
        def _():
            lax.fori_loop(sent(t - 1), sent(t), emit_own, 0)

        @pl.when(z != w)
        def _():
            lax.fori_loop(received(t - 1), received(t), pass_on, 0)

        @pl.when(inbound)
        def _():
            lax.fori_loop(stray_received(t - 1), stray_received(t), take_stray, 0)
            far = t - pieces - 2
            near = t - pieces - early - 2
            near_x = jnp.where(side == 0, t - 2 * (pieces + scale), near)
            near_y = jnp.where(side == 1, t - 2 * pieces - 2, near)

            @pl.when((far >= 0) & (far < jnp.where(side == 0, early, pieces)))
            def _():
                spread_far(far)

            @pl.when((side == 0) & (far >= 0) & (far < early))
            def _():
                spread_far(far + early)

            @pl.when((depth > 1) & (near_y >= 0) & (near_y < pieces))
            def _():
                spread_near(1, yq, near_y)

            @pl.when((depth > 2) & (near_x >= 0) & (near_x < pieces))
            def _():
                spread_near(2, xq, near_x)

        @pl.when(outer & (depth == 1) & (t >= pieces) & (t < 2 * pieces))
        def _():
            j = t - pieces
            send(row_piece(xq, core, j), stray_piece(1, j), tx.at[7], rx_stray.at[1, j], onward_dev)

        @pl.when(outer & (depth == 2) & (side == 0) & (t >= 2 * (pieces - scale)) & (t < 2 * (pieces - scale) + early))
        def _():
            for shift in range(2):
                j = 2 * (t - 2 * (pieces - scale)) + shift
                send(row_piece(w, core, j), stray_piece(2, j), tx.at[7], rx_stray.at[2, j], onward_dev)

        turn = t - pieces - early - 2 * scale - 2

        @pl.when(relay & (turn >= 0) & (turn < early))
        def _():
            for way, chip, lone_at, x_side, here in ((0, 0, 1, 2, has_down), (1, 3, 0, 1, has_up)):
                @pl.when(here)
                def _():
                    j = turn + jnp.where(w == x_side, 0, early)
                    ref = stray_piece(way, j)
                    arrived(ref, rx_stray.at[way, j])
                    send_col(ref, late_slot(chip, core), j, 10 + way, (z, 2 * chip + lone_at))

        def load(task):
            m, kind = task // kinds, task % kinds
            quarter = jnp.where(m < 2, w, jnp.where(m < 4, xq, jnp.where(m < 6, yq, dq)))
            shard, way = 2 * quarter + m % 2, task % 2
            copy = pltpu.make_async_copy(rowbuf.at[shard, kind], stage.at[way], stage_sem.at[way])
            return copy, way, kind * panel_rows + shard * shard_rows

        def convert(task, carry):
            copy, way, start = load(task)

            @pl.when((task == 0) | (task == 6 * kinds))
            def _():
                copy.start()

            @pl.when((task + 1 != 6 * kinds) & (task + 1 < 8 * kinds))
            def _():
                load(task + 1)[0].start()

            copy.wait()
            split_into(stage[way], row_lead, row_trail, pl.multiple_of(start, shard_rows))
            return carry

        def converted(t):
            near_tasks = clip((t - pieces) * 8 // scale, 6 * kinds)
            return near_tasks + clip((t - pieces - early) * 4 // scale, 2 * kinds)

        lax.fori_loop(converted(t - 1), converted(t), convert, 0)
        ready = done(t)
        lax.fori_loop(carry, ready, quantum, 0)
        carry = ready
        return carry

    lax.fori_loop(0, last + 3 * scale, step, 0)

    def drain(slot, ref):
        pltpu.make_async_copy(ref, ref, tx.at[slot]).wait()

    def drain_shards(slot, count, condition):
        @pl.when(condition)
        def _():
            drain(slot, rowbuf.at[pl.ds(0, count)])

    drain(0, rowbuf.at[0])
    drain(1, rowbuf.at[0])
    drain(2, rowbuf.at[0, pl.ds(0, kinds // 2)])
    drain(3, rowbuf.at[0, pl.ds(0, kinds // 2)])
    drain(4, rowbuf.at[pl.ds(0, 4)])
    drain_shards(5, 3, has_up & (z >= w))
    drain_shards(6, 3, has_down & (z <= w))
    for count in (1, 2, 3):
        drain_shards(7, count, outer & (depth == count - 1))
        drain_shards(8, count, outer & (depth == count))
    drain_shards(9, 1, lone)
    for way, here in ((0, has_down), (1, has_up)):
        @pl.when(relay & here)
        def _():
            drain(10 + way, rowbuf.at[0, pl.ds(0, kinds // 2)])


def panels(response_coeffs, occupied_coeffs):
    perturbations, shard_rows, orbitals = response_coeffs.shape
    kinds = perturbations + 1
    pieces = kinds * CUTS
    any_space = pl.BlockSpec(memory_space=pl.ANY)
    float32, bfloat16 = jnp.float32, jnp.bfloat16
    return pl.pallas_call(
        panel_kernel,
        out_shape=(
            pltpu.VMEM((perturbations, 8 * shard_rows, 4 * shard_rows), float32),
            jax.ShapeDtypeStruct((8, kinds, shard_rows, orbitals), float32),
            jax.ShapeDtypeStruct((5, kinds, shard_rows, orbitals), float32),
            jax.ShapeDtypeStruct((3, kinds, shard_rows, orbitals), float32),
        ),
        in_specs=[any_space] * 2,
        out_specs=(pl.BlockSpec(memory_space=pltpu.VMEM),) + (any_space,) * 3,
        scratch_shapes=[
            pltpu.VMEM((kinds * 8 * shard_rows, orbitals), bfloat16),
            pltpu.VMEM((kinds * 8 * shard_rows, orbitals), bfloat16),
            pltpu.VMEM((shard_rows, orbitals), bfloat16),
            pltpu.VMEM((shard_rows, orbitals), bfloat16),
            pltpu.VMEM((2, shard_rows, orbitals), float32),
            pltpu.SemaphoreType.DMA((8, pieces)),
            pltpu.SemaphoreType.DMA((5, pieces)),
            pltpu.SemaphoreType.DMA((3, pieces)),
            pltpu.SemaphoreType.DMA((12,)),
            pltpu.SemaphoreType.DMA((kinds,)),
        ],
        compiler_params=pltpu.CompilerParams(
            collective_id=0, has_side_effects=True, vmem_limit_bytes=41_300_000
        ),
    )(response_coeffs, occupied_coeffs)[0]


def store_kernel(held, out, sem):
    rows = held.shape[1] // STORES
    copies = []
    for k in range(held.shape[0]):
        for part in range(STORES):
            at = pl.ds(part * rows, rows)
            copies.append(pltpu.make_async_copy(held.at[k, at], out.at[k, at], sem.at[k, part]))
    for copy in copies:
        copy.start()
    for copy in copies:
        copy.wait()


def store(held):
    return pl.pallas_call(
        store_kernel,
        out_shape=jax.ShapeDtypeStruct(held.shape, held.dtype),
        in_specs=[pl.BlockSpec(memory_space=pltpu.VMEM)],
        out_specs=pl.BlockSpec(memory_space=pl.ANY),
        scratch_shapes=[pltpu.SemaphoreType.DMA((held.shape[0], STORES))],
        compiler_params=pltpu.CompilerParams(vmem_limit_bytes=1_000_000),
    )(held)


def solution(mesh):
    fits = mesh.shape["row"] == 4 and mesh.shape["col"] == 8
    return jax.shard_map(
        (lambda *args: store(panels(*args))) if fits else shards,
        mesh=mesh,
        in_specs=(P(None, ("row", "col"), None), P(("row", "col"), None)),
        out_specs=P(None, "row", "col"),
        check_vma=False,
    )
```
